32 devices in a mesh: grp: 4 (over z), seq: 4 (over y, core), tp: 2 (over x).
Axes of the slice: x: 2, y: 2, z: 4, core: 2. Of those that a mesh axis runs over, the one named last changes fastest.
Arguments:
- queries: bfloat16 [2048, 8192], P(('grp', 'seq', 'tp')), may hold values from -108 to 108
- key_rows: bfloat16 [2048, 1024], P(('grp', 'seq', 'tp')), may hold values from -4 to 4
- value_rows: bfloat16 [2048, 1024], P(('grp', 'seq', 'tp')), may hold values from -6 to 6
- image_lengths: int32 [4, 4], P('grp'), may hold values from 1 to 256, 512 in all within a row
- block_table: int32 [16, 4], P(('grp', 'seq')), may hold values from 0 to 3, as said below
Outputs:
- attended: bfloat16 [2048, 8192], P(('grp', 'seq'), 'tp')
The draws below stay inside these ranges and needn't reach their ends.
Inputs may be any that keep to these rules, and one draw needn't show every extreme that they name: `block_table`: for each shard index and each group, exactly one block of each encoder group's shard is destined to that group.
All inputs are finite; a program needn't handle non-finite values.
Results may differ from the reference program's by a relative error of at most 0.004.
Values may be sent and summed in bfloat16 or wider, within the bound.
A program may use at most 64 MiB of HBM per device.

```python
import math
import jax
import jax.numpy as jnp
import numpy as np
from jax import lax

HEADS = 64
KVH = 8
HD = 128
IMGS = 4
GROUPS = 4
SHARDS = 4
SEQ = 512
ROWS = 2048
BLOCK = 32


def shared_draw(key):
    base_key = jax.random.fold_in(key, 811)
    key_values = jnp.clip(jax.random.normal(jax.random.fold_in(base_key, 1), (ROWS, KVH * HD), jnp.float32), -4.0, 4.0)
    return key_values


def draw_queries(key, part):
    drawn = jnp.clip(jax.random.normal(jax.random.fold_in(key, 977), (ROWS, HEADS * HD), jnp.float32), -6.0, 6.0)
    return drawn.astype(jnp.bfloat16)


def draw_key_rows(key, part):
    key_values = shared_draw(key)
    return key_values.astype(jnp.bfloat16)


def draw_block_table(key, part):

    def one_shard(shard_index):
        inner_key = jax.random.fold_in(key, 97 + shard_index)
        row_order = jax.random.permutation(jax.random.fold_in(inner_key, 1), GROUPS)
        column_order = jax.random.permutation(jax.random.fold_in(inner_key, 2), GROUPS)
        return (row_order[:, None] + column_order[None, :]) % GROUPS
    latin_rows = jax.vmap(one_shard)(jnp.arange(SHARDS, dtype=jnp.int32))
    return latin_rows.transpose(1, 0, 2).reshape(GROUPS * SHARDS, GROUPS).astype(jnp.int32)


def level_of(rng, shape, pieces, low, top_value):
    level = 1.0
    for dim, parts in pieces:
        steps = jax.random.uniform(jax.random.fold_in(jax.random.fold_in(rng, 6), dim), (parts,), jnp.float32, low / len(pieces), top_value / len(pieces))
        level = level * jnp.repeat(jnp.exp(steps), shape[dim] // parts).reshape((-1,) + (1,) * (len(shape) - 1 - dim))
    return level


def length_profile(number_of, total, reach, lean):
    loads = [(1 << 20) // math.isqrt(standing ** lean) + 1 for standing in range(2, number_of + 1)]
    surplus, holding = total - reach - (number_of - 1), [1] * (number_of - 1)
    while surplus > 0:
        free = [i for i in range(number_of - 1) if holding[i] < reach]
        mass, budget = sum([loads[i] for i in free]), surplus
        for i in free:
            addition = min(reach - holding[i], max(1, budget * loads[i] // mass), surplus)
            holding[i] = holding[i] + addition
            surplus = surplus - addition
    return np.array([reach] + holding)


def ragged_sizes(key, number_of, total, reach, lean):
    if number_of == 2:
        one = jax.random.randint(key, (), max(1, total - reach), min(reach, total - 1) + 1)
        return jnp.stack([one, total - one])
    tallies = jnp.asarray(length_profile(number_of, total, reach, lean), jnp.int32)
    couples = (number_of - 1) // 2
    donor, sink = tallies[1:1 + 2 * couples:2], tallies[2:2 + 2 * couples:2]
    slack = jnp.minimum(donor - 1, reach - sink)
    shifted = jax.random.randint(jax.random.fold_in(key, 1), (couples,), 0, 1 << 20) % (slack + 1)
    tallies = tallies.at[1:1 + 2 * couples:2].set(donor - shifted).at[2:2 + 2 * couples:2].set(sink + shifted)
    return tallies[jax.random.permutation(jax.random.fold_in(key, 2), number_of)]


def centred(stream_key, dims, deviation, limit, shards=(), kind=jnp.bfloat16):
    loudness = level_of(stream_key, dims, shards, -0.22, 0.18) if shards else 1.0
    values = jax.random.normal(stream_key, dims, jnp.float32) * deviation * loudness
    return jnp.minimum(jnp.maximum(values, -limit), limit).astype(kind)


def setup_inputs(seed: int = 0) -> dict:
    keys = jax.random.split(jax.random.key(seed), 6)
    queries = draw_queries(jax.random.fold_in(keys[5], 71), 0)
    key_rows = draw_key_rows(jax.random.fold_in(keys[5], 71), 0)
    value_rows = centred(keys[2], (ROWS, KVH * HD), 1.0, 6.0, ((0, 32),))
    image_lengths = jax.vmap(lambda own: ragged_sizes(own, IMGS, SEQ, SEQ // 2, 2))(jax.random.split(keys[3], GROUPS)).reshape((GROUPS, IMGS)).astype(jnp.int32)
    block_table = draw_block_table(jax.random.fold_in(keys[5], 71), 0)
    return dict(queries=queries, key_rows=key_rows, value_rows=value_rows, image_lengths=image_lengths, block_table=block_table)


MASKED_SCORE = -1e+30

def place_rows(matrix, chosen, width):
    blocks = matrix.reshape(GROUPS, SHARDS, GROUPS, BLOCK, width)
    source_ids = jnp.arange(GROUPS, dtype=jnp.int32)[None, :, None]
    shard_ids = jnp.arange(SHARDS, dtype=jnp.int32)[None, None, :]
    picked = blocks[source_ids, shard_ids, chosen]
    return picked.transpose(0, 2, 1, 3, 4).reshape(GROUPS, SEQ, width)

def group_attention(packed):
    query_group, key_group, value_group, lengths_row = packed
    position = jnp.arange(SEQ, dtype=jnp.int32)
    bounds = jnp.cumsum(lengths_row)[:-1].astype(jnp.int32)
    image_id = lax.optimization_barrier(jnp.sum((position[:, None] >= bounds[None, :]).astype(jnp.int32), axis=1))
    visible = (position[None, :] <= position[:, None]) & (image_id[None, :] == image_id[:, None])
    query_split = query_group.reshape(SEQ, KVH, HEADS // KVH, HD).transpose(1, 0, 2, 3)
    key_split = key_group.reshape(SEQ, KVH, HD).transpose(1, 0, 2)
    value_split = value_group.reshape(SEQ, KVH, HD).transpose(1, 0, 2)
    score_scale = 1.0 / math.sqrt(HD)

    def head_group(members):
        query_head, key_head, value_head = members
        scores = jnp.einsum('prd,md->rpm', query_head.astype(jnp.float32), key_head.astype(jnp.float32)) * score_scale
        masked = jnp.where(visible[None], scores, MASKED_SCORE)
        row_peak = lax.optimization_barrier(jnp.max(masked, axis=2, keepdims=True))
        weights = jnp.where(visible[None], jnp.exp(masked - row_peak), 0.0)
        summed = lax.optimization_barrier(jnp.sum(weights, axis=2))
        rounded = lax.optimization_barrier(weights.astype(jnp.bfloat16)).astype(jnp.float32)
        product = jnp.einsum('rpm,md->rpd', rounded, value_head.astype(jnp.float32))
        return product / summed[..., None]
    outputs = lax.map(head_group, (query_split, key_split, value_split))
    return outputs.transpose(2, 0, 1, 3).reshape(SEQ, HEADS * HD).astype(jnp.bfloat16)

def reference(queries, key_rows, value_rows, image_lengths, block_table):
    layout = block_table.reshape(GROUPS, SHARDS, GROUPS)
    slot_ids = jnp.arange(GROUPS, dtype=jnp.int32)
    matches = layout[None] == slot_ids[:, None, None, None]
    chosen = lax.optimization_barrier(jnp.sum(jnp.where(matches, slot_ids[None, None, None, :], 0), axis=3)).astype(jnp.int32)
    placed_q = place_rows(queries, chosen, HEADS * HD)
    placed_k = place_rows(key_rows, chosen, KVH * HD)
    placed_v = place_rows(value_rows, chosen, KVH * HD)
    result = lax.map(group_attention, (placed_q, placed_k, placed_v, image_lengths))
    return result.reshape(ROWS, HEADS * HD)
```

```python
import functools
import math

import jax
import jax.numpy as jnp
from jax import lax
from jax.experimental import pallas as pl
from jax.experimental.pallas import tpu as pltpu
from jax.sharding import PartitionSpec as P

HD = 128
MASKED = -1e30
MESH = pl.DeviceIdType.MESH


def partner(index, offset, size):
    offset = jnp.int32(offset)
    if size & (size - 1):
        return lax.rem(index + offset, size)
    result = jnp.int32(0)
    weight = 1
    while weight < size:
        mine, other = lax.rem(index // weight, 2), lax.rem(offset // weight, 2)
        result = result + weight * (mine + other - 2 * mine * other)
        weight *= 2
    return result


def kernel(sizes, q_in, k_in, v_in, lengths, table, out, *scratch):
    (groups, shard_count, tps, per, block, q_width, kv_width, pieces, ratio) = sizes
    local_rows = groups * block
    count = len(pieces)
    k_pieces = [j for j in range(count) if pieces[j][0] == 0]
    v_pieces = [j for j in range(count) if pieces[j][0] == 1]
    q_pieces = [j for j in range(count) if pieces[j][0] == 2]
    q_chunks = len(q_pieces)
    starts = [pieces[j][1] for j in q_pieces]
    chunks = [pieces[j][2] for j in q_pieces]
    stage = scratch[0:3]
    gathered = scratch[3 : 3 + count]
    packed = scratch[3 + count : 3 + 2 * count]
    q_recv = scratch[3 + 2 * count : 3 + 2 * count + q_chunks]
    rest = 3 + 2 * count + q_chunks
    (k_all, v_all, obuf, bias_ref) = scratch[rest : rest + 4]
    (load_sem, own_sem, xs_sem, xr_sem, zs_sem, zr_sem, ys_sem, yr_sem, out_sem) = scratch[
        rest + 4 :
    ]
    g = lax.axis_index("grp")
    s = lax.axis_index("seq")
    t = lax.axis_index("tp")

    inputs = (k_in, v_in, q_in)

    def source(j):
        which, offset, width = pieces[j]
        return which, width, offset

    def part_width(which):
        return q_width if which == 2 else kv_width

    loads = [pltpu.make_async_copy(inputs[i], stage[i], load_sem.at[i]) for i in range(3)]
    own = []
    for j in range(count):
        which, width, offset = source(j)
        lanes = pl.ds(pl.multiple_of(t * part_width(which) + offset, HD), width)
        own.append(
            pltpu.make_async_copy(
                inputs[which].at[:, :, lanes],
                gathered[j].at[pl.ds(t * per, per)],
                own_sem.at[j],
            )
        )
    for copy in loads:
        copy.start()
    for copy in own:
        copy.start()

    barrier = pltpu.get_barrier_semaphore()
    for d in range(1, tps):
        pl.semaphore_signal(
            barrier, inc=1, device_id={"tp": partner(t, d, tps)}, device_id_type=MESH
        )
    for d in range(1, shard_count):
        pl.semaphore_signal(
            barrier, inc=1, device_id={"seq": partner(s, d, shard_count)}, device_id_type=MESH
        )
    for d in range(1, groups):
        pl.semaphore_signal(
            barrier, inc=1, device_id={"grp": partner(g, d, groups)}, device_id_type=MESH
        )
    pl.semaphore_wait(barrier, tps + shard_count + groups - 3)

    def x_copy(j, d):
        which, width, offset = source(j)
        peer = partner(t, d, tps)
        lanes = pl.ds(pl.multiple_of(peer * part_width(which) + offset, HD), width)
        return pltpu.make_async_remote_copy(
            src_ref=stage[which].at[:, :, lanes],
            dst_ref=gathered[j].at[pl.ds(t * per, per)],
            send_sem=xs_sem.at[j, d],
            recv_sem=xr_sem.at[j, d],
            device_id={"tp": peer},
            device_id_type=MESH,
        )

    for j in range(count):
        which, offset, _ = pieces[j]
        if offset == 0:
            loads[which].wait()
        for d in range(1, tps):
            x_copy(j, d).start()

    order = list(range(1, groups))
    held_back = [d for d in order if d >= 3 * groups // 4]
    chosen = []
    for d in [0] + order:
        dest = partner(g, d, groups)
        pick = jnp.int32(0)
        for b in range(groups):
            pick = jnp.where(table[0, b] == dest, b, pick)
        chosen.append(pick)

    def landing(j, group):
        which, offset, width = pieces[j]
        if which == 2:
            return q_recv[j - q_pieces[0]].at[group]
        return (k_all, v_all)[which].at[s, group, :, pl.ds(offset, width)]

    def z_copy(j, d):
        return pltpu.make_async_remote_copy(
            src_ref=packed[j].at[d],
            dst_ref=landing(j, g),
            send_sem=zs_sem.at[j, d],
            recv_sem=zr_sem.at[j, d],
            device_id={"grp": partner(g, d, groups)},
            device_id_type=MESH,
        )

    def hand_over(j):
        own[j].wait()
        for d in range(1, tps):
            x_copy(j, d).wait_recv()
        for d, pick in zip(order, chosen[1:]):
            packed[j][d] = gathered[j][pick]
        for d in order:
            if j not in q_pieces or d not in held_back:
                z_copy(j, d).start()
        landing(j, g)[...] = gathered[j][chosen[0]]

    def arrived(j):
        for d in range(1, groups):
            z_copy(j, d).wait_recv()

    relayed = shard_count % 2 == 0 and shard_count & (shard_count - 1) == 0

    def y_copy(i, d, slot, to):
        whole = (k_all, v_all)[i]
        return pltpu.make_async_remote_copy(
            src_ref=whole.at[slot],
            dst_ref=whole.at[slot],
            send_sem=ys_sem.at[i, d],
            recv_sem=yr_sem.at[i, d],
            device_id={"seq": partner(s, to, shard_count)},
            device_id_type=MESH,
        )

    def direct(d):
        return not relayed or d % 2 == 0 or d == 1

    def y_any(i, d):
        if direct(d):
            return y_copy(i, d, s, d)
        return y_copy(i, d, partner(s, d - 1, shard_count), 1)

    def spread(i):
        for j in (k_pieces, v_pieces)[i]:
            arrived(j)
        for d in range(shard_count - 1, 0, -1):
            if direct(d):
                y_any(i, d).start()

    def relay(i):
        for d in range(shard_count - 1, 0, -1):
            if not direct(d):
                y_any(i, d - 1).wait_recv()
                y_any(i, d).start()

    for j in k_pieces + v_pieces + q_pieces[:1]:
        hand_over(j)

    keys = shard_count * local_rows
    query_pos = s * local_rows + lax.broadcasted_iota(jnp.int32, (local_rows, keys), 0)
    key_pos = lax.broadcasted_iota(jnp.int32, (local_rows, keys), 1)
    query_img = jnp.zeros((local_rows, keys), jnp.int32)
    key_img = jnp.zeros((local_rows, keys), jnp.int32)
    bound = jnp.int32(0)
    for i in range(lengths.shape[1] - 1):
        bound = bound + lengths[0, i]
        query_img = query_img + (query_pos >= bound).astype(jnp.int32)
        key_img = key_img + (key_pos >= bound).astype(jnp.int32)
    visible = (key_pos <= query_pos) & (query_img == key_img)
    bias_ref[...] = jnp.where(visible, 0.0, MASKED)

    spread(0)
    for j in q_pieces[1:3]:
        hand_over(j)
    spread(1)
    for j in q_pieces[3:4]:
        hand_over(j)
    relay(0)
    for j in q_pieces[4:5]:
        hand_over(j)
    relay(1)
    for j in q_pieces[5:]:
        hand_over(j)
    for j in q_pieces:
        for d in held_back:
            z_copy(j, d).start()
    for i in range(2):
        for d in range(1, shard_count):
            if not direct(d) or d == 1 or not relayed:
                y_any(i, d).wait_recv()

    factor = math.log2(math.e) / math.sqrt(HD)

    def out_copy(n):
        return pltpu.make_async_copy(
            obuf.at[:, pl.ds(starts[n], chunks[n])],
            out.at[:, pl.ds(starts[n], chunks[n])],
            out_sem.at[n],
        )

    for n in range(q_chunks):
        arrived(q_pieces[n])
        for r in range(chunks[n] // HD):
            head = starts[n] // HD + r
            kv = head // ratio
            key = k_all[:, :, :, kv * HD : (kv + 1) * HD].reshape(keys, HD)
            value = v_all[:, :, :, kv * HD : (kv + 1) * HD].reshape(keys, HD)
            query = q_recv[n][:, :, r * HD : (r + 1) * HD].reshape(local_rows, HD)
            scores = lax.dot_general(
                query, key, (((1,), (1,)), ((), ())), preferred_element_type=jnp.float32
            )
            masked = scores + bias_ref[...]
            peak = jnp.max(masked, axis=1, keepdims=True)
            weights = jnp.exp2((masked - peak) * factor)
            summed = jnp.sum(weights, axis=1, keepdims=True)
            product = jnp.dot(
                weights.astype(jnp.bfloat16), value, preferred_element_type=jnp.float32
            )
            obuf[:, head * HD : (head + 1) * HD] = (product / summed).astype(jnp.bfloat16)
        out_copy(n).start()

    for j in range(count):
        for d in range(1, tps):
            x_copy(j, d).wait_send()
        for d in range(1, groups):
            z_copy(j, d).wait_send()
    for i in range(2):
        for d in range(1, shard_count):
            y_any(i, d).wait_send()
    for n in range(q_chunks):
        out_copy(n).wait()


def chunk_widths(heads, step):
    return [HD * min(step, heads - at) for at in range(0, heads, step)]


def growing(width):
    pieces = []
    at, size = 0, HD
    while at < width:
        size = min(size, width - at)
        pieces.append((at, size))
        at += size
        size = at
    return pieces


def shards(queries, key_rows, value_rows, image_lengths, block_table):
    groups, shard_count, tps = (lax.axis_size(a) for a in ("grp", "seq", "tp"))
    rows, q_total = queries.shape
    kv_total = key_rows.shape[1]
    local_rows = rows * tps
    block = local_rows // groups
    per = rows // block
    q_width, kv_width = q_total // tps, kv_total // tps
    ratio = q_total // kv_total
    chunks = chunk_widths(q_width // HD, max(1, ratio // 2))
    q_chunks = len(chunks)
    pieces = [(0, a, w) for a, w in growing(kv_width)]
    pieces.append((1, 0, kv_width))
    pieces += [(2, sum(chunks[:n]), w) for n, w in enumerate(chunks)]
    count = len(pieces)
    sizes = (groups, shard_count, tps, per, block, q_width, kv_width, tuple(pieces), ratio)
    bf16 = jnp.bfloat16
    widths = [w for _, _, w in pieces]
    dma = pltpu.SemaphoreType.DMA
    scratch = (
        [pltpu.VMEM((per, block, w), bf16) for w in (kv_total, kv_total, q_total)]
        + [pltpu.VMEM((groups, block, w), bf16) for w in widths]
        + [pltpu.VMEM((groups, block, w), bf16) for w in widths]
        + [pltpu.VMEM((groups, block, w), bf16) for w in chunks]
        + [
            pltpu.VMEM((shard_count, groups, block, kv_width), bf16),
            pltpu.VMEM((shard_count, groups, block, kv_width), bf16),
            pltpu.VMEM((local_rows, q_width), bf16),
            pltpu.VMEM((local_rows, shard_count * local_rows), jnp.float32),
            dma((3,)),
            dma((count,)),
            dma((count, tps)),
            dma((count, tps)),
            dma((count, groups)),
            dma((count, groups)),
            dma((2, shard_count)),
            dma((2, shard_count)),
            dma((q_chunks,)),
        ]
    )
    hbm = pl.BlockSpec(memory_space=pl.ANY)
    smem = pl.BlockSpec(memory_space=pltpu.SMEM)
    return pl.pallas_call(
        functools.partial(kernel, sizes),
        out_shape=jax.ShapeDtypeStruct((local_rows, q_width), bf16),
        in_specs=[hbm, hbm, hbm, smem, smem],
        out_specs=hbm,
        scratch_shapes=scratch,
        compiler_params=pltpu.CompilerParams(collective_id=0, has_side_effects=True),
    )(
        queries.reshape(per, block, q_total),
        key_rows.reshape(per, block, kv_total),
        value_rows.reshape(per, block, kv_total),
        image_lengths,
        block_table,
    )


def solution(mesh):
    in_specs = (
        P(("grp", "seq", "tp"), None),
        P(("grp", "seq", "tp"), None),
        P(("grp", "seq", "tp"), None),
        P("grp", None),
        P(("grp", "seq"), None),
    )
    out_specs = P(("grp", "seq"), "tp")
    return jax.shard_map(shards, mesh=mesh, in_specs=in_specs, out_specs=out_specs, check_vma=False)
```

```python
import functools
import math

import jax
import jax.numpy as jnp
from jax import lax
from jax.experimental import pallas as pl
from jax.experimental.pallas import tpu as pltpu
from jax.sharding import PartitionSpec as P

HD = 128
MASKED = -1e30
MESH = pl.DeviceIdType.MESH


def partner(index, offset, size):
    offset = jnp.int32(offset)
    if size & (size - 1):
        return lax.rem(index + offset, size)
    result = jnp.int32(0)
    weight = 1
    while weight < size:
        mine, other = lax.rem(index // weight, 2), lax.rem(offset // weight, 2)
        result = result + weight * (mine + other - 2 * mine * other)
        weight *= 2
    return result


def kernel(sizes, q_in, k_in, v_in, lengths, table, out, *scratch):
    (groups, shard_count, tps, per, block, q_width, kv_width, pieces, ratio) = sizes
    local_rows = groups * block
    count = len(pieces)
    k_pieces = [j for j in range(count) if pieces[j][0] == 0]
    v_pieces = [j for j in range(count) if pieces[j][0] == 1]
    q_pieces = [j for j in range(count) if pieces[j][0] == 2]
    q_chunks = len(q_pieces)
    starts = [pieces[j][1] for j in q_pieces]
    chunks = [pieces[j][2] for j in q_pieces]
    stage = scratch[0:3]
    gathered = scratch[3 : 3 + count]
    packed = scratch[3 + count : 3 + 2 * count]
    q_recv = scratch[3 + 2 * count : 3 + 2 * count + q_chunks]
    rest = 3 + 2 * count + q_chunks
    (k_all, v_all, obuf, bias_ref) = scratch[rest : rest + 4]
    (load_sem, own_sem, xs_sem, xr_sem, zs_sem, zr_sem, ys_sem, yr_sem, out_sem) = scratch[
        rest + 4 :
    ]
    g = lax.axis_index("grp")
    s = lax.axis_index("seq")
    t = lax.axis_index("tp")

    inputs = (k_in, v_in, q_in)

    def source(j):
        which, offset, width = pieces[j]
        return which, width, offset

    def part_width(which):
        return q_width if which == 2 else kv_width

    loads = [pltpu.make_async_copy(inputs[i], stage[i], load_sem.at[i]) for i in range(3)]
    own = []
    for j in range(count):
        which, width, offset = source(j)
        lanes = pl.ds(pl.multiple_of(t * part_width(which) + offset, HD), width)
        own.append(
            pltpu.make_async_copy(
                inputs[which].at[:, :, lanes],
                gathered[j].at[pl.ds(t * per, per)],
                own_sem.at[j],
            )
        )
    for copy in loads:
        copy.start()
    for copy in own:
        copy.start()

    barrier = pltpu.get_barrier_semaphore()
    for d in range(1, tps):
        pl.semaphore_signal(
            barrier, inc=1, device_id={"tp": partner(t, d, tps)}, device_id_type=MESH
        )
    for d in range(1, shard_count):
        pl.semaphore_signal(
            barrier, inc=1, device_id={"seq": partner(s, d, shard_count)}, device_id_type=MESH
        )
    for d in range(1, groups):
        pl.semaphore_signal(
            barrier, inc=1, device_id={"grp": partner(g, d, groups)}, device_id_type=MESH
        )
    pl.semaphore_wait(barrier, tps + shard_count + groups - 3)

    def x_copy(j, d):
        which, width, offset = source(j)
        peer = partner(t, d, tps)
        lanes = pl.ds(pl.multiple_of(peer * part_width(which) + offset, HD), width)
        return pltpu.make_async_remote_copy(
            src_ref=stage[which].at[:, :, lanes],
            dst_ref=gathered[j].at[pl.ds(t * per, per)],
            send_sem=xs_sem.at[j, d],
            recv_sem=xr_sem.at[j, d],
            device_id={"tp": peer},
            device_id_type=MESH,
        )

    for j in range(count):
        which, offset, _ = pieces[j]
        if offset == 0:
            loads[which].wait()
        for d in range(1, tps):
            x_copy(j, d).start()

    order = list(range(1, groups))
    held_back = [d for d in order if d >= 3 * groups // 4]
    chosen = []
    for d in [0] + order:
        dest = partner(g, d, groups)
        pick = jnp.int32(0)
        for b in range(groups):
            pick = jnp.where(table[0, b] == dest, b, pick)
        chosen.append(pick)

    def landing(j, group):
        which, offset, width = pieces[j]
        if which == 2:
            return q_recv[j - q_pieces[0]].at[group]
        return (k_all, v_all)[which].at[s, group, :, pl.ds(offset, width)]

    def z_copy(j, d):
        return pltpu.make_async_remote_copy(
            src_ref=packed[j].at[d],
            dst_ref=landing(j, g),
            send_sem=zs_sem.at[j, d],
            recv_sem=zr_sem.at[j, d],
            device_id={"grp": partner(g, d, groups)},
            device_id_type=MESH,
        )

    def hand_over(j):
        own[j].wait()
        for d in range(1, tps):
            x_copy(j, d).wait_recv()
        for d, pick in zip(order, chosen[1:]):
            packed[j][d] = gathered[j][pick]
        for d in order:
            if j not in q_pieces or d not in held_back:
                z_copy(j, d).start()
        landing(j, g)[...] = gathered[j][chosen[0]]

    def arrived(j):
        for d in range(1, groups):
            z_copy(j, d).wait_recv()

    relayed = shard_count % 2 == 0 and shard_count & (shard_count - 1) == 0

    def y_copy(i, d, slot, to):
        whole = (k_all, v_all)[i]
        return pltpu.make_async_remote_copy(
            src_ref=whole.at[slot],
            dst_ref=whole.at[slot],
            send_sem=ys_sem.at[i, d],
            recv_sem=yr_sem.at[i, d],
            device_id={"seq": partner(s, to, shard_count)},
            device_id_type=MESH,
        )

    def direct(d):
        return not relayed or d % 2 == 0 or d == 1

    def y_any(i, d):
        if direct(d):
            return y_copy(i, d, s, d)
        return y_copy(i, d, partner(s, d - 1, shard_count), 1)

    def spread(i):
        for j in (k_pieces, v_pieces)[i]:
            arrived(j)
        for d in range(shard_count - 1, 0, -1):
            if direct(d):
                y_any(i, d).start()

    def relay(i):
        for d in range(shard_count - 1, 0, -1):
            if not direct(d):
                y_any(i, d - 1).wait_recv()
                y_any(i, d).start()

    for j in k_pieces + v_pieces + q_pieces[:1]:
        hand_over(j)

    keys = shard_count * local_rows
    query_pos = s * local_rows + lax.broadcasted_iota(jnp.int32, (local_rows, keys), 0)
    key_pos = lax.broadcasted_iota(jnp.int32, (local_rows, keys), 1)
    query_img = jnp.zeros((local_rows, keys), jnp.int32)
    key_img = jnp.zeros((local_rows, keys), jnp.int32)
    bound = jnp.int32(0)
    for i in range(lengths.shape[1] - 1):
        bound = bound + lengths[0, i]
        query_img = query_img + (query_pos >= bound).astype(jnp.int32)
        key_img = key_img + (key_pos >= bound).astype(jnp.int32)
    visible = (key_pos <= query_pos) & (query_img == key_img)
    bias_ref[...] = jnp.where(visible, 0.0, MASKED)

    spread(0)
    for j in q_pieces[1:3]:
        hand_over(j)
    spread(1)
    for j in q_pieces[3:4]:
        hand_over(j)
    relay(0)
    for j in q_pieces[4:5]:
        hand_over(j)
    relay(1)
    for j in q_pieces[5:]:
        hand_over(j)
    for j in q_pieces:
        for d in held_back:
            z_copy(j, d).start()
    for i in range(2):
        for d in range(1, shard_count):
            if not direct(d) or d == 1 or not relayed:
                y_any(i, d).wait_recv()

    factor = math.log2(math.e) / math.sqrt(HD)

    def out_copy(n):
        return pltpu.make_async_copy(
            obuf.at[:, pl.ds(starts[n], chunks[n])],
            out.at[:, pl.ds(starts[n], chunks[n])],
            out_sem.at[n],
        )

    for n in range(q_chunks):
        arrived(q_pieces[n])
        for r in range(chunks[n] // HD):
            head = starts[n] // HD + r
            kv = head // ratio
            key = k_all[:, :, :, kv * HD : (kv + 1) * HD].reshape(keys, HD)
            value = v_all[:, :, :, kv * HD : (kv + 1) * HD].reshape(keys, HD)
            query = q_recv[n][:, :, r * HD : (r + 1) * HD].reshape(local_rows, HD)
            scores = lax.dot_general(
                query, key, (((1,), (1,)), ((), ())), preferred_element_type=jnp.float32
            )
            masked = scores + bias_ref[...]
            peak = jnp.max(masked, axis=1, keepdims=True)
            weights = jnp.exp2((masked - peak) * factor).astype(jnp.bfloat16)
            extended = jnp.concatenate([value, jnp.ones_like(value)], axis=1)
            product = jnp.dot(weights, extended, preferred_element_type=jnp.float32)
            obuf[:, head * HD : (head + 1) * HD] = (product[:, :HD] / product[:, HD:]).astype(
                jnp.bfloat16
            )
        out_copy(n).start()

    for j in range(count):
        for d in range(1, tps):
            x_copy(j, d).wait_send()
        for d in range(1, groups):
            z_copy(j, d).wait_send()
    for i in range(2):
        for d in range(1, shard_count):
            y_any(i, d).wait_send()
    for n in range(q_chunks):
        out_copy(n).wait()


def chunk_widths(heads, step):
    return [HD * min(step, heads - at) for at in range(0, heads, step)]


def growing(width):
    pieces = []
    at, size = 0, HD
    while at < width:
        size = min(size, width - at)
        pieces.append((at, size))
        at += size
        size = at
    return pieces


def shards(queries, key_rows, value_rows, image_lengths, block_table):
    groups, shard_count, tps = (lax.axis_size(a) for a in ("grp", "seq", "tp"))
    rows, q_total = queries.shape
    kv_total = key_rows.shape[1]
    local_rows = rows * tps
    block = local_rows // groups
    per = rows // block
    q_width, kv_width = q_total // tps, kv_total // tps
    ratio = q_total // kv_total
    chunks = chunk_widths(q_width // HD, max(1, ratio // 2))
    q_chunks = len(chunks)
    pieces = [(0, a, w) for a, w in growing(kv_width)]
    pieces.append((1, 0, kv_width))
    pieces += [(2, sum(chunks[:n]), w) for n, w in enumerate(chunks)]
    count = len(pieces)
    sizes = (groups, shard_count, tps, per, block, q_width, kv_width, tuple(pieces), ratio)
    bf16 = jnp.bfloat16
    widths = [w for _, _, w in pieces]
    dma = pltpu.SemaphoreType.DMA
    scratch = (
        [pltpu.VMEM((per, block, w), bf16) for w in (kv_total, kv_total, q_total)]
        + [pltpu.VMEM((groups, block, w), bf16) for w in widths]
        + [pltpu.VMEM((groups, block, w), bf16) for w in widths]
        + [pltpu.VMEM((groups, block, w), bf16) for w in chunks]
        + [
            pltpu.VMEM((shard_count, groups, block, kv_width), bf16),
            pltpu.VMEM((shard_count, groups, block, kv_width), bf16),
            pltpu.VMEM((local_rows, q_width), bf16),
            pltpu.VMEM((local_rows, shard_count * local_rows), jnp.float32),
            dma((3,)),
            dma((count,)),
            dma((count, tps)),
            dma((count, tps)),
            dma((count, groups)),
            dma((count, groups)),
            dma((2, shard_count)),
            dma((2, shard_count)),
            dma((q_chunks,)),
        ]
    )
    hbm = pl.BlockSpec(memory_space=pl.ANY)
    smem = pl.BlockSpec(memory_space=pltpu.SMEM)
    return pl.pallas_call(
        functools.partial(kernel, sizes),
        out_shape=jax.ShapeDtypeStruct((local_rows, q_width), bf16),
        in_specs=[hbm, hbm, hbm, smem, smem],
        out_specs=hbm,
        scratch_shapes=scratch,
        compiler_params=pltpu.CompilerParams(collective_id=0, has_side_effects=True),
    )(
        queries.reshape(per, block, q_total),
        key_rows.reshape(per, block, kv_total),
        value_rows.reshape(per, block, kv_total),
        image_lengths,
        block_table,
    )


def solution(mesh):
    in_specs = (
        P(("grp", "seq", "tp"), None),
        P(("grp", "seq", "tp"), None),
        P(("grp", "seq", "tp"), None),
        P("grp", None),
        P(("grp", "seq"), None),
    )
    out_specs = P(("grp", "seq"), "tp")
    return jax.shard_map(shards, mesh=mesh, in_specs=in_specs, out_specs=out_specs, check_vma=False)
```

```python
import functools
import math

import jax
import jax.numpy as jnp
from jax import lax
from jax.experimental import pallas as pl
from jax.experimental.pallas import tpu as pltpu
from jax.sharding import PartitionSpec as P

HD = 128
MASKED = -1e30
MESH = pl.DeviceIdType.MESH


def partner(index, offset, size):
    offset = jnp.int32(offset)
    if size & (size - 1):
        return lax.rem(index + offset, size)
    result = jnp.int32(0)
    weight = 1
    while weight < size:
        mine, other = lax.rem(index // weight, 2), lax.rem(offset // weight, 2)
        result = result + weight * (mine + other - 2 * mine * other)
        weight *= 2
    return result


def kernel(sizes, q_in, k_in, v_in, lengths, table, out, *scratch):
    (groups, shard_count, tps, per, block, q_width, kv_width, pieces, ratio) = sizes
    local_rows = groups * block
    count = len(pieces)
    k_pieces = [j for j in range(count) if pieces[j][0] == 0]
    v_pieces = [j for j in range(count) if pieces[j][0] == 1]
    q_pieces = [j for j in range(count) if pieces[j][0] == 2]
    q_chunks = len(q_pieces)
    starts = [pieces[j][1] for j in q_pieces]
    chunks = [pieces[j][2] for j in q_pieces]
    stage = scratch[0:3]
    gathered = scratch[3 : 3 + count]
    packed = scratch[3 + count : 3 + 2 * count]
    q_recv = scratch[3 + 2 * count : 3 + 2 * count + q_chunks]
    rest = 3 + 2 * count + q_chunks
    (k_all, v_all, bias_ref) = scratch[rest : rest + 3]
    (load_sem, own_sem, xs_sem, xr_sem, zs_sem, zr_sem, ys_sem, yr_sem) = scratch[rest + 3 :]
    g = lax.axis_index("grp")
    s = lax.axis_index("seq")
    t = lax.axis_index("tp")

    inputs = (k_in, v_in, q_in)

    def source(j):
        which, offset, width = pieces[j]
        return which, width, offset

    def part_width(which):
        return q_width if which == 2 else kv_width

    loads = [pltpu.make_async_copy(inputs[i], stage[i], load_sem.at[i]) for i in range(3)]
    own = []
    for j in range(count):
        which, width, offset = source(j)
        lanes = pl.ds(pl.multiple_of(t * part_width(which) + offset, HD), width)
        own.append(
            pltpu.make_async_copy(
                inputs[which].at[:, :, lanes],
                gathered[j].at[pl.ds(t * per, per)],
                own_sem.at[j],
            )
        )
    for copy in loads:
        copy.start()
    for copy in own:
        copy.start()

    barrier = pltpu.get_barrier_semaphore()
    for d in range(1, tps):
        pl.semaphore_signal(
            barrier, inc=1, device_id={"tp": partner(t, d, tps)}, device_id_type=MESH
        )
    for d in range(1, shard_count):
        pl.semaphore_signal(
            barrier, inc=1, device_id={"seq": partner(s, d, shard_count)}, device_id_type=MESH
        )
    for d in range(1, groups):
        pl.semaphore_signal(
            barrier, inc=1, device_id={"grp": partner(g, d, groups)}, device_id_type=MESH
        )
    pl.semaphore_wait(barrier, tps + shard_count + groups - 3)

    def x_copy(j, d):
        which, width, offset = source(j)
        peer = partner(t, d, tps)
        lanes = pl.ds(pl.multiple_of(peer * part_width(which) + offset, HD), width)
        return pltpu.make_async_remote_copy(
            src_ref=stage[which].at[:, :, lanes],
            dst_ref=gathered[j].at[pl.ds(t * per, per)],
            send_sem=xs_sem.at[j, d],
            recv_sem=xr_sem.at[j, d],
            device_id={"tp": peer},
            device_id_type=MESH,
        )

    for j in range(count):
        which, offset, _ = pieces[j]
        if offset == 0:
            loads[which].wait()
        for d in range(1, tps):
            x_copy(j, d).start()

    order = list(range(1, groups))
    held_back = [d for d in order if d >= 3 * groups // 4]
    chosen = []
    for d in [0] + order:
        dest = partner(g, d, groups)
        pick = jnp.int32(0)
        for b in range(groups):
            pick = jnp.where(table[0, b] == dest, b, pick)
        chosen.append(pick)

    def landing(j, group):
        which, offset, width = pieces[j]
        if which == 2:
            return q_recv[j - q_pieces[0]].at[group]
        return (k_all, v_all)[which].at[s, group, :, pl.ds(offset, width)]

    def z_copy(j, d):
        return pltpu.make_async_remote_copy(
            src_ref=packed[j].at[d],
            dst_ref=landing(j, g),
            send_sem=zs_sem.at[j, d],
            recv_sem=zr_sem.at[j, d],
            device_id={"grp": partner(g, d, groups)},
            device_id_type=MESH,
        )

    def hand_over(j):
        own[j].wait()
        for d in range(1, tps):
            x_copy(j, d).wait_recv()
        for d, pick in zip(order, chosen[1:]):
            packed[j][d] = gathered[j][pick]
        for d in order:
            if j not in q_pieces or d not in held_back:
                z_copy(j, d).start()
        landing(j, g)[...] = gathered[j][chosen[0]]

    def arrived(j):
        for d in range(1, groups):
            z_copy(j, d).wait_recv()

    relayed = shard_count % 2 == 0 and shard_count & (shard_count - 1) == 0

    def y_copy(i, d, slot, to):
        whole = (k_all, v_all)[i]
        return pltpu.make_async_remote_copy(
            src_ref=whole.at[slot],
            dst_ref=whole.at[slot],
            send_sem=ys_sem.at[i, d],
            recv_sem=yr_sem.at[i, d],
            device_id={"seq": partner(s, to, shard_count)},
            device_id_type=MESH,
        )

    def direct(d):
        return not relayed or d % 2 == 0 or d == 1

    def y_any(i, d):
        if direct(d):
            return y_copy(i, d, s, d)
        return y_copy(i, d, partner(s, d - 1, shard_count), 1)

    def spread(i):
        for j in (k_pieces, v_pieces)[i]:
            arrived(j)
        for d in range(shard_count - 1, 0, -1):
            if direct(d):
                y_any(i, d).start()

    def relay(i):
        for d in range(shard_count - 1, 0, -1):
            if not direct(d):
                y_any(i, d - 1).wait_recv()
                y_any(i, d).start()

    for j in k_pieces + v_pieces + q_pieces[:1]:
        hand_over(j)

    keys = shard_count * local_rows
    query_pos = s * local_rows + lax.broadcasted_iota(jnp.int32, (local_rows, keys), 0)
    key_pos = lax.broadcasted_iota(jnp.int32, (local_rows, keys), 1)
    query_img = jnp.zeros((local_rows, keys), jnp.int32)
    key_img = jnp.zeros((local_rows, keys), jnp.int32)
    bound = jnp.int32(0)
    for i in range(lengths.shape[1] - 1):
        bound = bound + lengths[0, i]
        query_img = query_img + (query_pos >= bound).astype(jnp.int32)
        key_img = key_img + (key_pos >= bound).astype(jnp.int32)
    visible = (key_pos <= query_pos) & (query_img == key_img)
    bias_ref[...] = jnp.where(visible, 0.0, MASKED)

    spread(0)
    for j in q_pieces[1:3]:
        hand_over(j)
    spread(1)
    for j in q_pieces[3:4]:
        hand_over(j)
    relay(0)
    for j in q_pieces[4:5]:
        hand_over(j)
    relay(1)
    for j in q_pieces[5:]:
        hand_over(j)
    for j in q_pieces:
        for d in held_back:
            z_copy(j, d).start()
    for i in range(2):
        for d in range(1, shard_count):
            if not direct(d) or d == 1 or not relayed:
                y_any(i, d).wait_recv()

    factor = math.log2(math.e) / math.sqrt(HD)

    for n in range(q_chunks):
        arrived(q_pieces[n])
        for r in range(chunks[n] // HD):
            head = starts[n] // HD + r
            kv = head // ratio
            key = k_all[:, :, :, kv * HD : (kv + 1) * HD].reshape(keys, HD)
            value = v_all[:, :, :, kv * HD : (kv + 1) * HD].reshape(keys, HD)
            query = q_recv[n][:, :, r * HD : (r + 1) * HD].reshape(local_rows, HD)
            scores = lax.dot_general(
                query, key, (((1,), (1,)), ((), ())), preferred_element_type=jnp.float32
            )
            masked = scores + bias_ref[...]
            peak = jnp.max(masked, axis=1, keepdims=True)
            weights = jnp.exp2((masked - peak) * factor).astype(jnp.bfloat16)
            extended = jnp.concatenate([value, jnp.ones_like(value)], axis=1)
            product = jnp.dot(weights, extended, preferred_element_type=jnp.float32)
            out[:, head * HD : (head + 1) * HD] = (product[:, :HD] / product[:, HD:]).astype(
                jnp.bfloat16
            )

    for j in range(count):
        for d in range(1, tps):
            x_copy(j, d).wait_send()
        for d in range(1, groups):
            z_copy(j, d).wait_send()
    for i in range(2):
        for d in range(1, shard_count):
            y_any(i, d).wait_send()


def chunk_widths(heads, step):
    return [HD * min(step, heads - at) for at in range(0, heads, step)]


def growing(width):
    pieces = []
    at, size = 0, HD
    while at < width:
        size = min(size, width - at)
        pieces.append((at, size))
        at += size
        size = at
    return pieces


def shards(queries, key_rows, value_rows, image_lengths, block_table):
    groups, shard_count, tps = (lax.axis_size(a) for a in ("grp", "seq", "tp"))
    rows, q_total = queries.shape
    kv_total = key_rows.shape[1]
    local_rows = rows * tps
    block = local_rows // groups
    per = rows // block
    q_width, kv_width = q_total // tps, kv_total // tps
    ratio = q_total // kv_total
    chunks = chunk_widths(q_width // HD, max(1, ratio // 2))
    q_chunks = len(chunks)
    pieces = [(0, a, w) for a, w in growing(kv_width)]
    pieces.append((1, 0, kv_width))
    pieces += [(2, sum(chunks[:n]), w) for n, w in enumerate(chunks)]
    count = len(pieces)
    sizes = (groups, shard_count, tps, per, block, q_width, kv_width, tuple(pieces), ratio)
    bf16 = jnp.bfloat16
    widths = [w for _, _, w in pieces]
    dma = pltpu.SemaphoreType.DMA
    scratch = (
        [pltpu.VMEM((per, block, w), bf16) for w in (kv_total, kv_total, q_total)]
        + [pltpu.VMEM((groups, block, w), bf16) for w in widths]
        + [pltpu.VMEM((groups, block, w), bf16) for w in widths]
        + [pltpu.VMEM((groups, block, w), bf16) for w in chunks]
        + [
            pltpu.VMEM((shard_count, groups, block, kv_width), bf16),
            pltpu.VMEM((shard_count, groups, block, kv_width), bf16),
            pltpu.VMEM((local_rows, shard_count * local_rows), jnp.float32),
            dma((3,)),
            dma((count,)),
            dma((count, tps)),
            dma((count, tps)),
            dma((count, groups)),
            dma((count, groups)),
            dma((2, shard_count)),
            dma((2, shard_count)),
        ]
    )
    hbm = pl.BlockSpec(memory_space=pl.ANY)
    smem = pl.BlockSpec(memory_space=pltpu.SMEM)
    return pl.pallas_call(
        functools.partial(kernel, sizes),
        out_shape=pltpu.VMEM((local_rows, q_width), bf16),
        in_specs=[hbm, hbm, hbm, smem, smem],
        out_specs=pl.BlockSpec(memory_space=pltpu.VMEM),
        scratch_shapes=scratch,
        compiler_params=pltpu.CompilerParams(collective_id=0, has_side_effects=True),
    )(
        queries.reshape(per, block, q_total),
        key_rows.reshape(per, block, kv_total),
        value_rows.reshape(per, block, kv_total),
        image_lengths,
        block_table,
    )


def solution(mesh):
    in_specs = (
        P(("grp", "seq", "tp"), None),
        P(("grp", "seq", "tp"), None),
        P(("grp", "seq", "tp"), None),
        P("grp", None),
        P(("grp", "seq"), None),
    )
    out_specs = P(("grp", "seq"), "tp")
    return jax.shard_map(shards, mesh=mesh, in_specs=in_specs, out_specs=out_specs, check_vma=False)
```

```python
import functools
import math

import jax
import jax.numpy as jnp
from jax import lax
from jax.experimental import pallas as pl
from jax.experimental.pallas import tpu as pltpu
from jax.sharding import PartitionSpec as P

HD = 128
MASKED = -1e30
MESH = pl.DeviceIdType.MESH


def partner(index, offset, size):
    offset = jnp.int32(offset)
    if size & (size - 1):
        return lax.rem(index + offset, size)
    result = jnp.int32(0)
    weight = 1
    while weight < size:
        mine, other = lax.rem(index // weight, 2), lax.rem(offset // weight, 2)
        result = result + weight * (mine + other - 2 * mine * other)
        weight *= 2
    return result


def origin(index, offset, size):
    return partner(index, size - offset if size & (size - 1) else offset, size)


def kernel(sizes, q_in, k_in, v_in, lengths, table, out, *scratch):
    (groups, shard_count, tps, per, block, q_width, kv_width, pieces, ratio) = sizes
    local_rows = groups * block
    count = len(pieces)
    k_pieces = [j for j in range(count) if pieces[j][0] == 0]
    v_pieces = [j for j in range(count) if pieces[j][0] == 1]
    q_pieces = [j for j in range(count) if pieces[j][0] == 2]
    q_chunks = len(q_pieces)
    starts = [pieces[j][1] for j in q_pieces]
    chunks = [pieces[j][2] for j in q_pieces]
    stage = scratch[0:3]
    gathered = scratch[3 : 3 + count]
    packed = scratch[3 + count : 3 + 2 * count]
    q_recv = scratch[3 + 2 * count : 3 + 2 * count + q_chunks]
    rest = 3 + 2 * count + q_chunks
    (k_all, v_all, bias_ref) = scratch[rest : rest + 3]
    (load_sem, own_sem, xs_sem, xr_sem, zs_sem, zr_sem, ys_sem, yr_sem, in_sem) = scratch[
        rest + 3 :
    ]
    g = lax.axis_index("grp")
    s = lax.axis_index("seq")
    t = lax.axis_index("tp")

    inputs = (k_in, v_in, q_in)

    def source(j):
        which, offset, width = pieces[j]
        return which, width, offset

    def part_width(which):
        return q_width if which == 2 else kv_width

    loads = [pltpu.make_async_copy(inputs[i], stage[i], load_sem.at[i]) for i in range(3)]
    own = []
    for j in range(count):
        which, width, offset = source(j)
        lanes = pl.ds(pl.multiple_of(t * part_width(which) + offset, HD), width)
        own.append(
            pltpu.make_async_copy(
                inputs[which].at[:, :, lanes],
                gathered[j].at[pl.ds(t * per, per)],
                own_sem.at[j],
            )
        )
    for copy in loads:
        copy.start()
    for copy in own:
        copy.start()

    relayed = shard_count % 2 == 0 and shard_count & (shard_count - 1) == 0

    def direct(d):
        return not relayed or d % 2 == 0 or d == 1

    seq_peers = [d for d in range(1, shard_count) if direct(d)]
    sides = [side for side in (1, -1) if groups > 1]

    def beyond(side):
        return groups - 1 - g if side == 1 else g

    barrier = pltpu.get_barrier_semaphore()
    for d in range(1, tps):
        pl.semaphore_signal(
            barrier, inc=1, device_id={"tp": partner(t, d, tps)}, device_id_type=MESH
        )
    for d in seq_peers:
        pl.semaphore_signal(
            barrier, inc=1, device_id={"seq": partner(s, d, shard_count)}, device_id_type=MESH
        )
    for side in sides:

        @pl.when(beyond(side) >= 1)
        def _(side=side):
            pl.semaphore_signal(
                barrier, inc=1, device_id={"grp": g + side}, device_id_type=MESH
            )

    met = jnp.int32(tps - 1 + len(seq_peers))
    for side in sides:
        met = met + (beyond(side) >= 1).astype(jnp.int32)
    pl.semaphore_wait(barrier, met)

    def pass_on(side, hops):
        @pl.when((beyond(side) >= hops) & (beyond(-side) >= 1))
        def _():
            pl.semaphore_signal(
                in_sem.at[(1 - side) // 2, hops + 1],
                inc=1,
                device_id={"grp": g - side},
                device_id_type=MESH,
            )

    def hear(side, hops):
        @pl.when(beyond(side) >= hops)
        def _():
            pl.semaphore_wait(in_sem.at[(1 - side) // 2, hops], 1)

    for side in sides:
        pass_on(side, 1)

    def x_copy(j, d):
        which, width, offset = source(j)
        peer = partner(t, d, tps)
        lanes = pl.ds(pl.multiple_of(peer * part_width(which) + offset, HD), width)
        return pltpu.make_async_remote_copy(
            src_ref=stage[which].at[:, :, lanes],
            dst_ref=gathered[j].at[pl.ds(t * per, per)],
            send_sem=xs_sem.at[j, d],
            recv_sem=xr_sem.at[j, d],
            device_id={"tp": peer},
            device_id_type=MESH,
        )

    for j in range(count):
        which, offset, _ = pieces[j]
        if offset == 0:
            loads[which].wait()
        for d in range(1, tps):
            x_copy(j, d).start()

    for hops in range(2, groups):
        for side in sides:
            hear(side, hops)
        for side in sides:
            pass_on(side, hops)

    order = list(range(1, groups))
    held_back = [d for d in order if d >= 3 * groups // 4]
    chosen = []
    for d in [0] + order:
        dest = partner(g, d, groups)
        pick = jnp.int32(0)
        for b in range(groups):
            pick = jnp.where(table[0, b] == dest, b, pick)
        chosen.append(pick)

    def landing(j, d):
        which, offset, width = pieces[j]
        if which == 2:
            return q_recv[j - q_pieces[0]].at[d]
        return (k_all, v_all)[which].at[s, g, :, pl.ds(offset, width)]

    def z_copy(j, d):
        return pltpu.make_async_remote_copy(
            src_ref=packed[j].at[d],
            dst_ref=landing(j, d),
            send_sem=zs_sem.at[j, d],
            recv_sem=zr_sem.at[j, d],
            device_id={"grp": partner(g, d, groups)},
            device_id_type=MESH,
        )

    def hand_over(j):
        own[j].wait()
        for d in range(1, tps):
            x_copy(j, d).wait_recv()
        for d, pick in zip(order, chosen[1:]):
            packed[j][d] = gathered[j][pick]
        for d in order:
            if j not in q_pieces or d not in held_back:
                z_copy(j, d).start()
        landing(j, 0)[...] = gathered[j][chosen[0]]

    def arrived(j, offsets=range(1, groups)):
        for d in offsets:
            z_copy(j, d).wait_recv()

    def y_copy(i, d, slot, to):
        whole = (k_all, v_all)[i]
        return pltpu.make_async_remote_copy(
            src_ref=whole.at[slot],
            dst_ref=whole.at[slot],
            send_sem=ys_sem.at[i, d],
            recv_sem=yr_sem.at[i, d],
            device_id={"seq": partner(s, to, shard_count)},
            device_id_type=MESH,
        )

    def y_any(i, d):
        if direct(d):
            return y_copy(i, d, s, d)
        return y_copy(i, d, partner(s, d - 1, shard_count), 1)

    def spread(i):
        for j in (k_pieces, v_pieces)[i]:
            arrived(j)
        for d in range(shard_count - 1, 0, -1):
            if direct(d):
                y_any(i, d).start()

    def relay(i):
        for d in range(shard_count - 1, 0, -1):
            if not direct(d):
                y_any(i, d - 1).wait_recv()
                y_any(i, d).start()

    keys = shard_count * local_rows
    row = lax.broadcasted_iota(jnp.int32, (block, keys), 0)
    query_pos = jnp.concatenate(
        [s * local_rows + origin(g, d, groups) * block + row for d in range(groups)], axis=0
    )
    key_pos = lax.broadcasted_iota(jnp.int32, (local_rows, keys), 1)
    query_img = jnp.zeros((local_rows, keys), jnp.int32)
    key_img = jnp.zeros((local_rows, keys), jnp.int32)
    bound = jnp.int32(0)
    for i in range(lengths.shape[1] - 1):
        bound = bound + lengths[0, i]
        query_img = query_img + (query_pos >= bound).astype(jnp.int32)
        key_img = key_img + (key_pos >= bound).astype(jnp.int32)
    visible = (key_pos <= query_pos) & (query_img == key_img)
    bias_ref[...] = jnp.where(visible, 0.0, MASKED)

    for j in k_pieces + v_pieces + q_pieces:
        hand_over(j)
    for j in q_pieces:
        for d in held_back:
            z_copy(j, d).start()
    spread(0)
    spread(1)
    relay(0)
    relay(1)
    for i in range(2):
        for d in range(1, shard_count):
            if not direct(d) or d == 1 or not relayed:
                y_any(i, d).wait_recv()

    factor = math.log2(math.e) / math.sqrt(HD)

    def attend(query, head, bias):
        lanes = slice(head // ratio * HD, (head // ratio + 1) * HD)
        key = k_all[:, :, :, lanes].reshape(keys, HD)
        value = v_all[:, :, :, lanes].reshape(keys, HD)
        scores = lax.dot_general(
            query, key, (((1,), (1,)), ((), ())), preferred_element_type=jnp.float32
        )
        masked = scores + bias
        peak = jnp.max(masked, axis=1, keepdims=True)
        weights = jnp.exp2((masked - peak) * factor).astype(jnp.bfloat16)
        extended = jnp.concatenate([value, jnp.ones_like(value)], axis=1)
        product = jnp.dot(weights, extended, preferred_element_type=jnp.float32)
        return (product[:, :HD] / product[:, HD:]).astype(jnp.bfloat16)

    def place(d, head, result):
        rows = pl.ds(pl.multiple_of(origin(g, d, groups) * block, block), block)
        out[rows, head * HD : (head + 1) * HD] = result

    prompt = [d for d in range(groups) if d not in held_back]
    for n in range(q_chunks):
        arrived(q_pieces[n], prompt[1:])
        for r in range(chunks[n] // HD):
            head = starts[n] // HD + r
            query = q_recv[n][: len(prompt), :, r * HD : (r + 1) * HD]
            result = attend(
                query.reshape(len(prompt) * block, HD), head, bias_ref[: len(prompt) * block]
            )
            for d in prompt:
                place(d, head, result[d * block : (d + 1) * block])

    batches = [range(n, min(n + 2, q_chunks)) for n in range(0, q_chunks, 2)]
    for batch in batches:
        for n in batch:
            arrived(q_pieces[n], held_back)
        spans = {}
        for n in batch:
            for r in range(chunks[n] // HD):
                head = starts[n] // HD + r
                spans.setdefault(head // ratio, []).append((n, r, head))
        for d in held_back:
            for members in spans.values():
                stack = [q_recv[n][d, :, r * HD : (r + 1) * HD] for n, r, _ in members]
                bias = bias_ref[d * block : (d + 1) * block]
                result = attend(
                    jnp.concatenate(stack, axis=0),
                    members[0][2],
                    jnp.concatenate([bias] * len(members), axis=0),
                )
                for i, (_, _, head) in enumerate(members):
                    place(d, head, result[i * block : (i + 1) * block])

    for j in range(count):
        for d in range(1, tps):
            x_copy(j, d).wait_send()
        for d in range(1, groups):
            z_copy(j, d).wait_send()
    for i in range(2):
        for d in range(1, shard_count):
            y_any(i, d).wait_send()


def chunk_widths(heads, step):
    return [HD * min(step, heads - at) for at in range(0, heads, step)]


def growing(width):
    pieces = []
    at, size = 0, HD
    while at < width:
        size = min(size, width - at)
        pieces.append((at, size))
        at += size
        size = at
    return pieces


def shards(queries, key_rows, value_rows, image_lengths, block_table):
    groups, shard_count, tps = (lax.axis_size(a) for a in ("grp", "seq", "tp"))
    rows, q_total = queries.shape
    kv_total = key_rows.shape[1]
    local_rows = rows * tps
    block = local_rows // groups
    per = rows // block
    q_width, kv_width = q_total // tps, kv_total // tps
    ratio = q_total // kv_total
    chunks = chunk_widths(q_width // HD, max(1, ratio // 2))
    q_chunks = len(chunks)
    pieces = [(0, a, w) for a, w in growing(kv_width)]
    pieces.append((1, 0, kv_width))
    pieces += [(2, sum(chunks[:n]), w) for n, w in enumerate(chunks)]
    count = len(pieces)
    sizes = (groups, shard_count, tps, per, block, q_width, kv_width, tuple(pieces), ratio)
    bf16 = jnp.bfloat16
    widths = [w for _, _, w in pieces]
    dma = pltpu.SemaphoreType.DMA
    scratch = (
        [pltpu.VMEM((per, block, w), bf16) for w in (kv_total, kv_total, q_total)]
        + [pltpu.VMEM((groups, block, w), bf16) for w in widths]
        + [pltpu.VMEM((groups, block, w), bf16) for w in widths]
        + [pltpu.VMEM((groups, block, w), bf16) for w in chunks]
        + [
            pltpu.VMEM((shard_count, groups, block, kv_width), bf16),
            pltpu.VMEM((shard_count, groups, block, kv_width), bf16),
            pltpu.VMEM((local_rows, shard_count * local_rows), jnp.float32),
            dma((3,)),
            dma((count,)),
            dma((count, tps)),
            dma((count, tps)),
            dma((count, groups)),
            dma((count, groups)),
            dma((2, shard_count)),
            dma((2, shard_count)),
            pltpu.SemaphoreType.REGULAR((2, groups + 1)),
        ]
    )
    hbm = pl.BlockSpec(memory_space=pl.ANY)
    smem = pl.BlockSpec(memory_space=pltpu.SMEM)
    return pl.pallas_call(
        functools.partial(kernel, sizes),
        out_shape=pltpu.VMEM((local_rows, q_width), bf16),
        in_specs=[hbm, hbm, hbm, smem, smem],
        out_specs=pl.BlockSpec(memory_space=pltpu.VMEM),
        scratch_shapes=scratch,
        compiler_params=pltpu.CompilerParams(collective_id=0, has_side_effects=True),
    )(
        queries.reshape(per, block, q_total),
        key_rows.reshape(per, block, kv_total),
        value_rows.reshape(per, block, kv_total),
        image_lengths,
        block_table,
    )


def solution(mesh):
    in_specs = (
        P(("grp", "seq", "tp"), None),
        P(("grp", "seq", "tp"), None),
        P(("grp", "seq", "tp"), None),
        P("grp", None),
        P(("grp", "seq"), None),
    )
    out_specs = P(("grp", "seq"), "tp")
    return jax.shard_map(shards, mesh=mesh, in_specs=in_specs, out_specs=out_specs, check_vma=False)
```

```python
import functools
import math

import jax
import jax.numpy as jnp
from jax import lax
from jax.experimental import pallas as pl
from jax.experimental.pallas import tpu as pltpu
from jax.sharding import PartitionSpec as P

HD = 128
MASKED = -1e30
MESH = pl.DeviceIdType.MESH


def partner(index, offset, size):
    offset = jnp.int32(offset)
    if size & (size - 1):
        return lax.rem(index + offset, size)
    result = jnp.int32(0)
    weight = 1
    while weight < size:
        mine, other = lax.rem(index // weight, 2), lax.rem(offset // weight, 2)
        result = result + weight * (mine + other - 2 * mine * other)
        weight *= 2
    return result


def origin(index, offset, size):
    return partner(index, size - offset if size & (size - 1) else offset, size)


def kernel(sizes, q_in, k_in, v_in, lengths, table, out, *scratch):
    (groups, shard_count, tps, per, block, q_width, kv_width, pieces, ratio) = sizes
    local_rows = groups * block
    count = len(pieces)
    k_pieces = [j for j in range(count) if pieces[j][0] == 0]
    v_pieces = [j for j in range(count) if pieces[j][0] == 1]
    q_pieces = [j for j in range(count) if pieces[j][0] == 2]
    q_chunks = len(q_pieces)
    starts = [pieces[j][1] for j in q_pieces]
    chunks = [pieces[j][2] for j in q_pieces]
    stage = scratch[0:3]
    gathered = scratch[3 : 3 + count]
    packed = scratch[3 + count : 3 + 2 * count]
    q_recv = scratch[3 + 2 * count : 3 + 2 * count + q_chunks]
    rest = 3 + 2 * count + q_chunks
    (k_all, v_all, bias_ref) = scratch[rest : rest + 3]
    (load_sem, own_sem, xs_sem, xr_sem, zs_sem, zr_sem, ys_sem, yr_sem, in_sem) = scratch[
        rest + 3 :
    ]
    g = lax.axis_index("grp")
    s = lax.axis_index("seq")
    t = lax.axis_index("tp")

    inputs = (k_in, v_in, q_in)

    def source(j):
        which, offset, width = pieces[j]
        return which, width, offset

    def part_width(which):
        return q_width if which == 2 else kv_width

    loads = [pltpu.make_async_copy(inputs[i], stage[i], load_sem.at[i]) for i in range(3)]
    own = []
    for j in range(count):
        which, width, offset = source(j)
        lanes = pl.ds(pl.multiple_of(t * part_width(which) + offset, HD), width)
        own.append(
            pltpu.make_async_copy(
                inputs[which].at[:, :, lanes],
                gathered[j].at[pl.ds(t * per, per)],
                own_sem.at[j],
            )
        )
    for copy in loads:
        copy.start()
    for copy in own:
        copy.start()

    relayed = shard_count % 2 == 0 and shard_count & (shard_count - 1) == 0

    def direct(d):
        return not relayed or d % 2 == 0 or d == 1

    seq_peers = [d for d in range(1, shard_count) if direct(d)]
    sides = [side for side in (1, -1) if groups > 1]

    def beyond(side):
        return groups - 1 - g if side == 1 else g

    barrier = pltpu.get_barrier_semaphore()
    for d in range(1, tps):
        pl.semaphore_signal(
            barrier, inc=1, device_id={"tp": partner(t, d, tps)}, device_id_type=MESH
        )
    for d in seq_peers:
        pl.semaphore_signal(
            barrier, inc=1, device_id={"seq": partner(s, d, shard_count)}, device_id_type=MESH
        )
    for side in sides:

        @pl.when(beyond(side) >= 1)
        def _(side=side):
            pl.semaphore_signal(
                barrier, inc=1, device_id={"grp": g + side}, device_id_type=MESH
            )

    met = jnp.int32(tps - 1 + len(seq_peers))
    for side in sides:
        met = met + (beyond(side) >= 1).astype(jnp.int32)
    pl.semaphore_wait(barrier, met)

    def pass_on(side, hops):
        @pl.when((beyond(side) >= hops) & (beyond(-side) >= 1))
        def _():
            pl.semaphore_signal(
                in_sem.at[(1 - side) // 2, hops + 1],
                inc=1,
                device_id={"grp": g - side},
                device_id_type=MESH,
            )

    def hear(side, hops):
        @pl.when(beyond(side) >= hops)
        def _():
            pl.semaphore_wait(in_sem.at[(1 - side) // 2, hops], 1)

    for side in sides:
        pass_on(side, 1)

    def x_copy(j, d):
        which, width, offset = source(j)
        peer = partner(t, d, tps)
        lanes = pl.ds(pl.multiple_of(peer * part_width(which) + offset, HD), width)
        return pltpu.make_async_remote_copy(
            src_ref=stage[which].at[:, :, lanes],
            dst_ref=gathered[j].at[pl.ds(t * per, per)],
            send_sem=xs_sem.at[j, d],
            recv_sem=xr_sem.at[j, d],
            device_id={"tp": peer},
            device_id_type=MESH,
        )

    for j in range(count):
        which, offset, _ = pieces[j]
        if offset == 0:
            loads[which].wait()
        for d in range(1, tps):
            x_copy(j, d).start()

    for hops in range(2, groups):
        for side in sides:
            hear(side, hops)
        for side in sides:
            pass_on(side, hops)

    held_back = [d for d in range(1, groups) if d >= 3 * groups // 4]
    order = [d for d in range(groups - 1, 0, -1) if d not in held_back] + held_back
    chosen = []
    for d in [0] + order:
        dest = partner(g, d, groups)
        pick = jnp.int32(0)
        for b in range(groups):
            pick = jnp.where(table[0, b] == dest, b, pick)
        chosen.append(pick)

    def landing(j, d):
        which, offset, width = pieces[j]
        if which == 2:
            return q_recv[j - q_pieces[0]].at[d]
        return (k_all, v_all)[which].at[s, g, :, pl.ds(offset, width)]

    def z_copy(j, d):
        return pltpu.make_async_remote_copy(
            src_ref=packed[j].at[d],
            dst_ref=landing(j, d),
            send_sem=zs_sem.at[j, d],
            recv_sem=zr_sem.at[j, d],
            device_id={"grp": partner(g, d, groups)},
            device_id_type=MESH,
        )

    def hand_over(j):
        own[j].wait()
        for d in range(1, tps):
            x_copy(j, d).wait_recv()
        for d, pick in zip(order, chosen[1:]):
            packed[j][d] = gathered[j][pick]
        for d in order:
            if j not in q_pieces or d not in held_back:
                z_copy(j, d).start()
        landing(j, 0)[...] = gathered[j][chosen[0]]

    def arrived(j, offsets=range(1, groups)):
        for d in offsets:
            z_copy(j, d).wait_recv()

    def y_copy(i, d, slot, to):
        whole = (k_all, v_all)[i]
        return pltpu.make_async_remote_copy(
            src_ref=whole.at[slot],
            dst_ref=whole.at[slot],
            send_sem=ys_sem.at[i, d],
            recv_sem=yr_sem.at[i, d],
            device_id={"seq": partner(s, to, shard_count)},
            device_id_type=MESH,
        )

    def y_any(i, d):
        if direct(d):
            return y_copy(i, d, s, d)
        return y_copy(i, d, partner(s, d - 1, shard_count), 1)

    def spread(i):
        for j in (k_pieces, v_pieces)[i]:
            arrived(j)
        for d in range(shard_count - 1, 0, -1):
            if direct(d):
                y_any(i, d).start()

    def relay(i):
        for d in range(shard_count - 1, 0, -1):
            if not direct(d):
                y_any(i, d - 1).wait_recv()
                y_any(i, d).start()

    keys = shard_count * local_rows
    row = lax.broadcasted_iota(jnp.int32, (block, keys), 0)
    query_pos = jnp.concatenate(
        [s * local_rows + origin(g, d, groups) * block + row for d in range(groups)], axis=0
    )
    key_pos = lax.broadcasted_iota(jnp.int32, (local_rows, keys), 1)
    query_img = jnp.zeros((local_rows, keys), jnp.int32)
    key_img = jnp.zeros((local_rows, keys), jnp.int32)
    bound = jnp.int32(0)
    for i in range(lengths.shape[1] - 1):
        bound = bound + lengths[0, i]
        query_img = query_img + (query_pos >= bound).astype(jnp.int32)
        key_img = key_img + (key_pos >= bound).astype(jnp.int32)
    visible = (key_pos <= query_pos) & (query_img == key_img)
    bias_ref[...] = jnp.where(visible, 0.0, MASKED)

    for j in k_pieces + v_pieces + q_pieces:
        hand_over(j)
    for j in q_pieces:
        for d in held_back:
            z_copy(j, d).start()
    spread(0)
    spread(1)
    relay(0)
    relay(1)
    for i in range(2):
        for d in range(1, shard_count):
            if not direct(d) or d == 1 or not relayed:
                y_any(i, d).wait_recv()

    factor = math.log2(math.e) / math.sqrt(HD)

    def attend(query, head, bias):
        lanes = slice(head // ratio * HD, (head // ratio + 1) * HD)
        key = k_all[:, :, :, lanes].reshape(keys, HD)
        value = v_all[:, :, :, lanes].reshape(keys, HD)
        scores = lax.dot_general(
            query, key, (((1,), (1,)), ((), ())), preferred_element_type=jnp.float32
        )
        masked = scores + bias
        peak = jnp.max(masked, axis=1, keepdims=True)
        weights = jnp.exp2((masked - peak) * factor).astype(jnp.bfloat16)
        extended = jnp.concatenate([value, jnp.ones_like(value)], axis=1)
        product = jnp.dot(weights, extended, preferred_element_type=jnp.float32)
        return (product[:, :HD] / product[:, HD:]).astype(jnp.bfloat16)

    def place(d, head, result):
        rows = pl.ds(pl.multiple_of(origin(g, d, groups) * block, block), block)
        out[rows, head * HD : (head + 1) * HD] = result

    prompt = [d for d in range(groups) if d not in held_back]
    for n in range(q_chunks):
        arrived(q_pieces[n], prompt[1:])
        for r in range(chunks[n] // HD):
            head = starts[n] // HD + r
            query = q_recv[n][: len(prompt), :, r * HD : (r + 1) * HD]
            result = attend(
                query.reshape(len(prompt) * block, HD), head, bias_ref[: len(prompt) * block]
            )
            for d in prompt:
                place(d, head, result[d * block : (d + 1) * block])

    batches = [range(n, min(n + 2, q_chunks)) for n in range(0, q_chunks, 2)]
    for batch in batches:
        for n in batch:
            arrived(q_pieces[n], held_back)
        spans = {}
        for n in batch:
            for r in range(chunks[n] // HD):
                head = starts[n] // HD + r
                spans.setdefault(head // ratio, []).append((n, r, head))
        for d in held_back:
            for members in spans.values():
                stack = [q_recv[n][d, :, r * HD : (r + 1) * HD] for n, r, _ in members]
                bias = bias_ref[d * block : (d + 1) * block]
                result = attend(
                    jnp.concatenate(stack, axis=0),
                    members[0][2],
                    jnp.concatenate([bias] * len(members), axis=0),
                )
                for i, (_, _, head) in enumerate(members):
                    place(d, head, result[i * block : (i + 1) * block])

    for j in range(count):
        for d in range(1, tps):
            x_copy(j, d).wait_send()
        for d in range(1, groups):
            z_copy(j, d).wait_send()
    for i in range(2):
        for d in range(1, shard_count):
            y_any(i, d).wait_send()


def chunk_widths(heads, step):
    return [HD * min(step, heads - at) for at in range(0, heads, step)]


def growing(width):
    pieces = []
    at, size = 0, HD
    while at < width:
        size = min(size, width - at)
        pieces.append((at, size))
        at += size
        size = at
    return pieces


def shards(queries, key_rows, value_rows, image_lengths, block_table):
    groups, shard_count, tps = (lax.axis_size(a) for a in ("grp", "seq", "tp"))
    rows, q_total = queries.shape
    kv_total = key_rows.shape[1]
    local_rows = rows * tps
    block = local_rows // groups
    per = rows // block
    q_width, kv_width = q_total // tps, kv_total // tps
    ratio = q_total // kv_total
    chunks = chunk_widths(q_width // HD, max(1, ratio // 2))
    q_chunks = len(chunks)
    pieces = [(0, a, w) for a, w in growing(kv_width)]
    pieces.append((1, 0, kv_width))
    pieces += [(2, sum(chunks[:n]), w) for n, w in enumerate(chunks)]
    count = len(pieces)
    sizes = (groups, shard_count, tps, per, block, q_width, kv_width, tuple(pieces), ratio)
    bf16 = jnp.bfloat16
    widths = [w for _, _, w in pieces]
    dma = pltpu.SemaphoreType.DMA
    scratch = (
        [pltpu.VMEM((per, block, w), bf16) for w in (kv_total, kv_total, q_total)]
        + [pltpu.VMEM((groups, block, w), bf16) for w in widths]
        + [pltpu.VMEM((groups, block, w), bf16) for w in widths]
        + [pltpu.VMEM((groups, block, w), bf16) for w in chunks]
        + [
            pltpu.VMEM((shard_count, groups, block, kv_width), bf16),
            pltpu.VMEM((shard_count, groups, block, kv_width), bf16),
            pltpu.VMEM((local_rows, shard_count * local_rows), jnp.float32),
            dma((3,)),
            dma((count,)),
            dma((count, tps)),
            dma((count, tps)),
            dma((count, groups)),
            dma((count, groups)),
            dma((2, shard_count)),
            dma((2, shard_count)),
            pltpu.SemaphoreType.REGULAR((2, groups + 1)),
        ]
    )
    hbm = pl.BlockSpec(memory_space=pl.ANY)
    smem = pl.BlockSpec(memory_space=pltpu.SMEM)
    return pl.pallas_call(
        functools.partial(kernel, sizes),
        out_shape=pltpu.VMEM((local_rows, q_width), bf16),
        in_specs=[hbm, hbm, hbm, smem, smem],
        out_specs=pl.BlockSpec(memory_space=pltpu.VMEM),
        scratch_shapes=scratch,
        compiler_params=pltpu.CompilerParams(collective_id=0, has_side_effects=True),
    )(
        queries.reshape(per, block, q_total),
        key_rows.reshape(per, block, kv_total),
        value_rows.reshape(per, block, kv_total),
        image_lengths,
        block_table,
    )


def solution(mesh):
    in_specs = (
        P(("grp", "seq", "tp"), None),
        P(("grp", "seq", "tp"), None),
        P(("grp", "seq", "tp"), None),
        P("grp", None),
        P(("grp", "seq"), None),
    )
    out_specs = P(("grp", "seq"), "tp")
    return jax.shard_map(shards, mesh=mesh, in_specs=in_specs, out_specs=out_specs, check_vma=False)
```

```python
import functools
import math

import jax
import jax.numpy as jnp
from jax import lax
from jax.experimental import pallas as pl
from jax.experimental.pallas import tpu as pltpu
from jax.sharding import PartitionSpec as P

HD = 128
MASKED = -1e30
MESH = pl.DeviceIdType.MESH


def partner(index, offset, size):
    offset = jnp.int32(offset)
    if size & (size - 1):
        return lax.rem(index + offset, size)
    result = jnp.int32(0)
    weight = 1
    while weight < size:
        mine, other = lax.rem(index // weight, 2), lax.rem(offset // weight, 2)
        result = result + weight * (mine + other - 2 * mine * other)
        weight *= 2
    return result


def origin(index, offset, size):
    return partner(index, size - offset if size & (size - 1) else offset, size)


def kernel(sizes, q_in, k_in, v_in, lengths, table, out, *scratch):
    (groups, shard_count, tps, per, block, q_width, kv_width, pieces, ratio) = sizes
    local_rows = groups * block
    count = len(pieces)
    k_pieces = [j for j in range(count) if pieces[j][0] == 0]
    v_pieces = [j for j in range(count) if pieces[j][0] == 1]
    q_pieces = [j for j in range(count) if pieces[j][0] == 2]
    q_chunks = len(q_pieces)
    starts = [pieces[j][1] for j in q_pieces]
    chunks = [pieces[j][2] for j in q_pieces]
    stage = scratch[0:3]
    gathered = scratch[3 : 3 + count]
    packed = scratch[3 + count : 3 + 2 * count]
    q_recv = scratch[3 + 2 * count : 3 + 2 * count + q_chunks]
    rest = 3 + 2 * count + q_chunks
    (k_all, v_all, bias_ref) = scratch[rest : rest + 3]
    (load_sem, own_sem, xs_sem, xr_sem, zs_sem, zr_sem, ys_sem, yr_sem, in_sem) = scratch[
        rest + 3 :
    ]
    g = lax.axis_index("grp")
    s = lax.axis_index("seq")
    t = lax.axis_index("tp")

    inputs = (k_in, v_in, q_in)

    def source(j):
        which, offset, width = pieces[j]
        return which, width, offset

    def part_width(which):
        return q_width if which == 2 else kv_width

    loads = [pltpu.make_async_copy(inputs[i], stage[i], load_sem.at[i]) for i in range(3)]
    own = []
    for j in range(count):
        which, width, offset = source(j)
        lanes = pl.ds(pl.multiple_of(t * part_width(which) + offset, HD), width)
        own.append(
            pltpu.make_async_copy(
                inputs[which].at[:, :, lanes],
                gathered[j].at[pl.ds(t * per, per)],
                own_sem.at[j],
            )
        )
    for copy in loads:
        copy.start()
    for copy in own:
        copy.start()

    relayed = shard_count % 2 == 0 and shard_count & (shard_count - 1) == 0

    def direct(d):
        return not relayed or d % 2 == 0 or d == 1

    seq_peers = [d for d in range(1, shard_count) if direct(d)]
    sides = [side for side in (1, -1) if groups > 1]

    def beyond(side):
        return groups - 1 - g if side == 1 else g

    barrier = pltpu.get_barrier_semaphore()
    for d in range(1, tps):
        pl.semaphore_signal(
            barrier, inc=1, device_id={"tp": partner(t, d, tps)}, device_id_type=MESH
        )
    for d in seq_peers:
        pl.semaphore_signal(
            barrier, inc=1, device_id={"seq": partner(s, d, shard_count)}, device_id_type=MESH
        )
    for side in sides:

        @pl.when(beyond(side) >= 1)
        def _(side=side):
            pl.semaphore_signal(
                barrier, inc=1, device_id={"grp": g + side}, device_id_type=MESH
            )

    met = jnp.int32(tps - 1 + len(seq_peers))
    for side in sides:
        met = met + (beyond(side) >= 1).astype(jnp.int32)
    pl.semaphore_wait(barrier, met)

    def pass_on(side, hops):
        @pl.when((beyond(side) >= hops) & (beyond(-side) >= 1))
        def _():
            pl.semaphore_signal(
                in_sem.at[(1 - side) // 2, hops + 1],
                inc=1,
                device_id={"grp": g - side},
                device_id_type=MESH,
            )

    def hear(side, hops):
        @pl.when(beyond(side) >= hops)
        def _():
            pl.semaphore_wait(in_sem.at[(1 - side) // 2, hops], 1)

    for side in sides:
        pass_on(side, 1)

    def x_copy(j, d):
        which, width, offset = source(j)
        peer = partner(t, d, tps)
        lanes = pl.ds(pl.multiple_of(peer * part_width(which) + offset, HD), width)
        return pltpu.make_async_remote_copy(
            src_ref=stage[which].at[:, :, lanes],
            dst_ref=gathered[j].at[pl.ds(t * per, per)],
            send_sem=xs_sem.at[j, d],
            recv_sem=xr_sem.at[j, d],
            device_id={"tp": peer},
            device_id_type=MESH,
        )

    for j in range(count):
        which, offset, _ = pieces[j]
        if offset == 0:
            loads[which].wait()
        for d in range(1, tps):
            x_copy(j, d).start()

    for hops in range(2, groups):
        for side in sides:
            hear(side, hops)
        for side in sides:
            pass_on(side, hops)

    held_back = [d for d in range(1, groups) if d >= 3 * groups // 4]
    order = [d for d in range(groups - 1, 0, -1) if d not in held_back] + held_back
    chosen = []
    for d in [0] + order:
        dest = partner(g, d, groups)
        pick = jnp.int32(0)
        for b in range(groups):
            pick = jnp.where(table[0, b] == dest, b, pick)
        chosen.append(pick)

    def landing(j, d):
        which, offset, width = pieces[j]
        if which == 2:
            return q_recv[j - q_pieces[0]].at[d]
        return (k_all, v_all)[which].at[s, g, :, pl.ds(offset, width)]

    def z_copy(j, d):
        return pltpu.make_async_remote_copy(
            src_ref=packed[j].at[d],
            dst_ref=landing(j, d),
            send_sem=zs_sem.at[j, d],
            recv_sem=zr_sem.at[j, d],
            device_id={"grp": partner(g, d, groups)},
            device_id_type=MESH,
        )

    def hand_over(j):
        own[j].wait()
        for d in range(1, tps):
            x_copy(j, d).wait_recv()
        for d, pick in zip(order, chosen[1:]):
            packed[j][d] = gathered[j][pick]
        for d in order:
            if j not in q_pieces or d not in held_back:
                z_copy(j, d).start()
        landing(j, 0)[...] = gathered[j][chosen[0]]

    def arrived(j, offsets=range(1, groups)):
        for d in offsets:
            z_copy(j, d).wait_recv()

    def y_copy(i, d, slot, to):
        whole = (k_all, v_all)[i]
        return pltpu.make_async_remote_copy(
            src_ref=whole.at[slot],
            dst_ref=whole.at[slot],
            send_sem=ys_sem.at[i, d],
            recv_sem=yr_sem.at[i, d],
            device_id={"seq": partner(s, to, shard_count)},
            device_id_type=MESH,
        )

    def y_any(i, d):
        if direct(d):
            return y_copy(i, d, s, d)
        return y_copy(i, d, partner(s, d - 1, shard_count), 1)

    def spread(i):
        for j in (k_pieces, v_pieces)[i]:
            arrived(j)
        for d in range(shard_count - 1, 0, -1):
            if direct(d):
                y_any(i, d).start()

    def relay(i):
        for d in range(shard_count - 1, 0, -1):
            if not direct(d):
                y_any(i, d - 1).wait_recv()
                y_any(i, d).start()

    keys = shard_count * local_rows
    row = lax.broadcasted_iota(jnp.int32, (block, keys), 0)
    query_pos = jnp.concatenate(
        [s * local_rows + origin(g, d, groups) * block + row for d in range(groups)], axis=0
    )
    key_pos = lax.broadcasted_iota(jnp.int32, (local_rows, keys), 1)
    query_img = jnp.zeros((local_rows, keys), jnp.int32)
    key_img = jnp.zeros((local_rows, keys), jnp.int32)
    bound = jnp.int32(0)
    for i in range(lengths.shape[1] - 1):
        bound = bound + lengths[0, i]
        query_img = query_img + (query_pos >= bound).astype(jnp.int32)
        key_img = key_img + (key_pos >= bound).astype(jnp.int32)
    visible = (key_pos <= query_pos) & (query_img == key_img)
    bias_ref[...] = jnp.where(visible, 0.0, MASKED)

    for j in k_pieces + v_pieces + q_pieces:
        hand_over(j)
    for j in q_pieces:
        for d in held_back:
            z_copy(j, d).start()
    spread(0)
    spread(1)
    relay(0)
    relay(1)
    for i in range(2):
        for d in range(1, shard_count):
            if not direct(d) or d == 1 or not relayed:
                y_any(i, d).wait_recv()

    factor = math.log2(math.e) / math.sqrt(HD)

    def attend(query, head, bias):
        lanes = slice(head // ratio * HD, (head // ratio + 1) * HD)
        key = k_all[:, :, :, lanes].reshape(keys, HD)
        value = v_all[:, :, :, lanes].reshape(keys, HD)
        scores = lax.dot_general(
            query, key, (((1,), (1,)), ((), ())), preferred_element_type=jnp.float32
        )
        masked = scores + bias
        peak = jnp.max(masked, axis=1, keepdims=True)
        weights = jnp.exp2((masked - peak) * factor).astype(jnp.bfloat16)
        extended = jnp.concatenate([value, jnp.ones_like(value)], axis=1)
        product = jnp.dot(weights, extended, preferred_element_type=jnp.float32)
        return (product[:, :HD] / product[:, HD:]).astype(jnp.bfloat16)

    def place(d, head, result):
        rows = pl.ds(pl.multiple_of(origin(g, d, groups) * block, block), block)
        out[rows, head * HD : (head + 1) * HD] = result

    prompt = [d for d in range(groups) if d not in held_back]
    for n in range(q_chunks):
        arrived(q_pieces[n], prompt[1:])
        for r in range(chunks[n] // HD):
            head = starts[n] // HD + r
            query = q_recv[n][: len(prompt), :, r * HD : (r + 1) * HD]
            result = attend(
                query.reshape(len(prompt) * block, HD), head, bias_ref[: len(prompt) * block]
            )
            for d in prompt:
                place(d, head, result[d * block : (d + 1) * block])

    batches = [range(n, min(n + 2, q_chunks)) for n in range(0, q_chunks, 2)]
    for batch in batches:
        for n in batch:
            arrived(q_pieces[n], held_back)
        spans = {}
        for n in batch:
            for r in range(chunks[n] // HD):
                head = starts[n] // HD + r
                spans.setdefault(head // ratio, []).append((n, r, head))
        for d in held_back:
            for members in spans.values():
                stack = [q_recv[n][d, :, r * HD : (r + 1) * HD] for n, r, _ in members]
                bias = bias_ref[d * block : (d + 1) * block]
                result = attend(
                    jnp.concatenate(stack, axis=0),
                    members[0][2],
                    jnp.concatenate([bias] * len(members), axis=0),
                )
                for i, (_, _, head) in enumerate(members):
                    place(d, head, result[i * block : (i + 1) * block])

    for j in range(count):
        for d in range(1, tps):
            x_copy(j, d).wait_send()
        for d in range(1, groups):
            z_copy(j, d).wait_send()
    for i in range(2):
        for d in range(1, shard_count):
            y_any(i, d).wait_send()


def chunk_widths(heads, step):
    return [HD * min(step, heads - at) for at in range(0, heads, step)]


def growing(width):
    pieces = []
    at, size = 0, HD
    while at < width:
        size = min(size, width - at)
        pieces.append((at, size))
        at += size
        size = width - at
    return pieces


def shards(queries, key_rows, value_rows, image_lengths, block_table):
    groups, shard_count, tps = (lax.axis_size(a) for a in ("grp", "seq", "tp"))
    rows, q_total = queries.shape
    kv_total = key_rows.shape[1]
    local_rows = rows * tps
    block = local_rows // groups
    per = rows // block
    q_width, kv_width = q_total // tps, kv_total // tps
    ratio = q_total // kv_total
    chunks = chunk_widths(q_width // HD, max(1, ratio // 2))
    q_chunks = len(chunks)
    pieces = [(0, a, w) for a, w in growing(kv_width)]
    pieces.append((1, 0, kv_width))
    pieces += [(2, sum(chunks[:n]), w) for n, w in enumerate(chunks)]
    count = len(pieces)
    sizes = (groups, shard_count, tps, per, block, q_width, kv_width, tuple(pieces), ratio)
    bf16 = jnp.bfloat16
    widths = [w for _, _, w in pieces]
    dma = pltpu.SemaphoreType.DMA
    scratch = (
        [pltpu.VMEM((per, block, w), bf16) for w in (kv_total, kv_total, q_total)]
        + [pltpu.VMEM((groups, block, w), bf16) for w in widths]
        + [pltpu.VMEM((groups, block, w), bf16) for w in widths]
        + [pltpu.VMEM((groups, block, w), bf16) for w in chunks]
        + [
            pltpu.VMEM((shard_count, groups, block, kv_width), bf16),
            pltpu.VMEM((shard_count, groups, block, kv_width), bf16),
            pltpu.VMEM((local_rows, shard_count * local_rows), jnp.float32),
            dma((3,)),
            dma((count,)),
            dma((count, tps)),
            dma((count, tps)),
            dma((count, groups)),
            dma((count, groups)),
            dma((2, shard_count)),
            dma((2, shard_count)),
            pltpu.SemaphoreType.REGULAR((2, groups + 1)),
        ]
    )
    hbm = pl.BlockSpec(memory_space=pl.ANY)
    smem = pl.BlockSpec(memory_space=pltpu.SMEM)
    return pl.pallas_call(
        functools.partial(kernel, sizes),
        out_shape=pltpu.VMEM((local_rows, q_width), bf16),
        in_specs=[hbm, hbm, hbm, smem, smem],
        out_specs=pl.BlockSpec(memory_space=pltpu.VMEM),
        scratch_shapes=scratch,
        compiler_params=pltpu.CompilerParams(collective_id=0, has_side_effects=True),
    )(
        queries.reshape(per, block, q_total),
        key_rows.reshape(per, block, kv_total),
        value_rows.reshape(per, block, kv_total),
        image_lengths,
        block_table,
    )


def solution(mesh):
    in_specs = (
        P(("grp", "seq", "tp"), None),
        P(("grp", "seq", "tp"), None),
        P(("grp", "seq", "tp"), None),
        P("grp", None),
        P(("grp", "seq"), None),
    )
    out_specs = P(("grp", "seq"), "tp")
    return jax.shard_map(shards, mesh=mesh, in_specs=in_specs, out_specs=out_specs, check_vma=False)
```
